32 devices in a mesh: parts: 2 (over y), brick: 4 (over z), rep: 2 (over x), sub: 2 (over core).
Axes of the slice: x: 2, y: 2, z: 4, core: 2. Of those that a mesh axis runs over, the one named last changes fastest.
Arguments:
- fine_cells: int32 [5, 32768], P(None, ('parts', 'brick', 'rep', 'sub')), parts along dimension 1, may hold values from 0 to 511, as said below
- fine_exponent: float32 [32768], P(('parts', 'brick', 'rep', 'sub')), parts along dimension 0, may hold values from 0.05 to 0.6
- fine_charge: float32 [32768], P(('parts', 'brick', 'rep', 'sub')), parts along dimension 0, may hold values from -6 to 6
- fine_offset: float32 [3, 32768], P(None, ('parts', 'brick', 'rep', 'sub')), parts along dimension 1, may hold values from 0 to 1
- wide_cells: int32 [5, 4096], P(None, ('parts', 'brick', 'rep', 'sub')), parts along dimension 1, may hold values from 0 to 127, as said below
- wide_exponent: float32 [4096], P(('parts', 'brick', 'rep', 'sub')), parts along dimension 0, may hold values from 0.05 to 0.6
- wide_charge: float32 [4096], P(('parts', 'brick', 'rep', 'sub')), parts along dimension 0, may hold values from -6 to 6
- wide_offset: float32 [3, 4096], P(None, ('parts', 'brick', 'rep', 'sub')), parts along dimension 1, may hold values from 0 to 1
Outputs:
- finest_grid: float32 [256, 512, 512], P(('parts', 'brick'), ('rep', 'sub')), parts along dimension 0
- second_grid: float32 [128, 256, 256], P(('parts', 'brick'), ('rep', 'sub')), parts along dimension 0
- middle_grid: float32 [64, 16384], P('parts', 'brick'), parts along dimension 0
- coarse_grid: float32 [32, 4096], P('parts', 'brick'), parts along dimension 0
- coarsest_grid: float32 [16, 1024], P('parts', 'brick'), parts along dimension 0
The draws below stay inside these ranges and needn't reach their ends.
There are 2 independent parts, one for each index of `parts`. The reference program is written for one: setup_inputs(seed, part) draws one part's arguments, and reference() takes and returns one part's arrays. A program takes and returns all parts, laid end to end along the dimension named above; each array names one. Nothing has to cross between parts.
Inputs may be any that keep to these rules, and one draw needn't show every extreme that they name: `fine_cells`: column n is one fine Gaussian: row 0 its level L (0 or 1), row 1 its radius (1 to 4, equal to 4 on every 16th column), rows 2 to 4 its centre cell on level L's grid. The centre lies in the block of the device that holds column n: along the first dimension within that device's brick block of 128/2^L/4 cells, along the second within its block of 512/2^L/4 cells along rep+sub, anywhere along the third. `wide_cells`: column n is one wide Gaussian: row 0 its level L (2 to 4), row 1 its radius (1 to 4, equal to 4 on every 16th column), rows 2 to 4 its centre cell, anywhere on level L's grid.
All inputs are finite; a program needn't handle non-finite values.
Results may differ from the reference program's by a relative error of at most 0.0038.
Values sent between devices are 32-bit elements; how exact they have to be, the bound alone decides.
A program may use at most 64 MiB of HBM per device.

```python
import math
import jax
import jax.numpy as jnp
from jax import lax

GRID = 512
ROWS = 128
HALF = 4
FINE_DEV = 1024
WIDE_DEV = 128
FINE = 16384
WIDE = 2048
N_BRICK = 4
N_REP = 2
N_SUB = 2


def draw_fine_cells(key, part):
    slot_count = FINE_DEV * N_BRICK * N_REP * N_SUB
    slots = jnp.arange(slot_count, dtype=jnp.int32)
    device = slots // FINE_DEV
    columns = N_REP * N_SUB
    brick_index = device // columns
    column_index = device % columns
    level_row = (jax.random.randint(jax.random.fold_in(key, 1), (slot_count,), 0, 4) == 0).astype(jnp.int32)
    radius = jax.random.randint(jax.random.fold_in(key, 2), (slot_count,), 1, HALF + 1)
    radius = jnp.where(slots % 16 == 0, HALF, radius)
    row_tile = jnp.right_shift(jnp.int32(ROWS), level_row) // N_BRICK
    period = jnp.right_shift(jnp.int32(GRID), level_row)
    col_tile = period // columns
    picks = jax.random.randint(jax.random.fold_in(key, 3), (3, slot_count), 0, 1 << 20)
    first_cell = brick_index * row_tile + picks[0] % row_tile
    second_cell = column_index * col_tile + picks[1] % col_tile
    third_cell = picks[2] % period
    return jnp.stack([level_row, radius, first_cell, second_cell, third_cell]).astype(jnp.int32)


def draw_wide_cells(key, part):
    slot_count = WIDE_DEV * N_BRICK * N_REP * N_SUB
    slots = jnp.arange(slot_count, dtype=jnp.int32)
    choose = jax.random.randint(jax.random.fold_in(key, 5), (slot_count,), 0, 8)
    level_row = jnp.where(slots % 8 == 3, 4, jnp.where(choose < 2, 3, 2)).astype(jnp.int32)
    radius = jax.random.randint(jax.random.fold_in(key, 6), (slot_count,), 1, HALF + 1)
    radius = jnp.where(slots % 16 == 0, HALF, radius)
    rows_here = jnp.right_shift(jnp.int32(ROWS), level_row)
    period = jnp.right_shift(jnp.int32(GRID), level_row)
    picks = jax.random.randint(jax.random.fold_in(key, 7), (3, slot_count), 0, 1 << 20)
    first_cell = picks[0] % rows_here
    second_cell = picks[1] % period
    third_cell = picks[2] % period
    return jnp.stack([level_row, radius, first_cell, second_cell, third_cell]).astype(jnp.int32)


def block_levels(key, shape, shards, least, high):
    loudness, own = 1.0, jax.random.fold_in(key, 6)
    for axis_at, parts in shards:
        draws = jnp.exp(jax.random.uniform(jax.random.fold_in(own, axis_at), (parts,), jnp.float32, least / len(shards), high / len(shards)))
        loudness = loudness * jnp.repeat(draws, shape[axis_at] // parts).reshape([-1 if axis == axis_at else 1 for axis in range(len(shape))])
    return loudness


def bell_draw(rng, dims, scale, reach, cuts=(), kind=jnp.bfloat16):
    drawn = jax.random.normal(rng, dims, jnp.float32) * scale
    if len(cuts) > 0:
        drawn = block_levels(rng, dims, cuts, -0.22, 0.18) * drawn
    return jnp.clip(drawn, min=-reach, max=reach).astype(kind)


def setup_inputs(seed: int = 0, part: int = 0) -> dict:
    splits = jax.random.split(jax.random.key(seed), 9)
    own_keys = jax.random.split(jax.random.fold_in(splits[8], part), 9)
    return {
        "fine_cells": draw_fine_cells(jax.random.fold_in(jax.random.fold_in(splits[8], part), 71), part),
        "fine_exponent": jnp.clip(jnp.exp(math.log(0.6) - 2.4849067 * jax.random.uniform(own_keys[1], (FINE,), jnp.float32) ** block_levels(own_keys[1], (FINE,), ((0, 16),), -0.2, 0.2)), 0.05, 0.6),
        "fine_charge": bell_draw(own_keys[2], (FINE,), 1.0, 6.0, ((0, 16),), jnp.float32),
        "fine_offset": jnp.clip(1.0 * jax.random.uniform(own_keys[3], (3, FINE), jnp.float32) ** block_levels(own_keys[3], (3, FINE), ((1, 16),), -0.2, 0.2), 0.0, 1.0),
        "wide_cells": draw_wide_cells(jax.random.fold_in(jax.random.fold_in(splits[8], part), 71), part),
        "wide_exponent": jnp.clip(jnp.exp(math.log(0.6) - 2.4849067 * jax.random.uniform(own_keys[5], (WIDE,), jnp.float32) ** block_levels(own_keys[5], (WIDE,), ((0, 16),), -0.2, 0.2)), 0.05, 0.6),
        "wide_charge": bell_draw(own_keys[6], (WIDE,), 1.0, 6.0, ((0, 16),), jnp.float32),
        "wide_offset": jnp.clip(1.0 * jax.random.uniform(own_keys[7], (3, WIDE), jnp.float32) ** block_levels(own_keys[7], (3, WIDE), ((1, 16),), -0.2, 0.2), 0.0, 1.0),
    }


def one_factor(offsets, radius, exponent, centre_shift):
    inside = jnp.abs(offsets) <= radius[:, None]
    spread = offsets.astype(exponent.dtype) - centre_shift[:, None]
    return jnp.where(inside, jnp.exp(-exponent[:, None] * spread * spread), 0.0)


def deposit(slot_table, exponent, charge, offset, first_level, level_count):
    base_list = []
    grid_cells = 0
    for level_index in range(first_level, first_level + level_count):
        base_list.append(grid_cells)
        grid_cells += (ROWS >> level_index) * (GRID >> level_index) ** 2
    base_table = jnp.array(base_list, dtype=jnp.int32)
    slot_count = slot_table.shape[1]
    batch_size = math.gcd(slot_count, 4096)
    span_cells = jnp.arange(-HALF, HALF + 1, dtype=jnp.int32)
    span_count = 2 * HALF + 1

    def add_batch(flat_grid, batch_index):
        first_slot = (batch_index * batch_size).astype(jnp.int32)
        part_table = lax.dynamic_slice_in_dim(slot_table, first_slot, batch_size, 1)
        part_exponent = lax.dynamic_slice_in_dim(exponent, first_slot, batch_size, 0)
        part_charge = lax.dynamic_slice_in_dim(charge, first_slot, batch_size, 0)
        part_offset = lax.dynamic_slice_in_dim(offset, first_slot, batch_size, 1)
        level_row = part_table[0]
        radius = part_table[1]
        rows_here = jnp.right_shift(jnp.int32(ROWS), level_row)
        period = jnp.right_shift(jnp.int32(GRID), level_row)
        base_cell = base_table[level_row - first_level]
        offsets = jnp.broadcast_to(span_cells[None, :], (batch_size, span_count))
        row_place = part_table[2][:, None] + span_cells[None, :]
        col_place = jnp.mod(part_table[3][:, None] + span_cells[None, :], period[:, None])
        depth_place = jnp.mod(part_table[4][:, None] + span_cells[None, :], period[:, None])
        row_factor = one_factor(offsets, radius, part_exponent, part_offset[0])
        col_factor = one_factor(offsets, radius, part_exponent, part_offset[1])
        depth_factor = one_factor(offsets, radius, part_exponent, part_offset[2])
        plane_weight = ((part_charge[:, None] * row_factor)[:, :, None] * col_factor[:, None, :]).astype(jnp.bfloat16)
        depth_weight = depth_factor.astype(jnp.bfloat16)
        values = plane_weight.astype(jnp.float32)[:, :, :, None] * depth_weight.astype(jnp.float32)[:, None, None, :]
        period_four = period[:, None, None, None]
        flat_index = base_cell[:, None, None, None] + (row_place[:, :, None, None] * period_four + col_place[:, None, :, None]) * period_four + depth_place[:, None, None, :]
        inside_window = (row_place >= 0) & (row_place < rows_here[:, None])
        flat_index = jnp.where(inside_window[:, :, None, None], flat_index, grid_cells).astype(jnp.int32)
        flat_grid = flat_grid.at[flat_index.reshape(-1)].add(values.reshape(-1), mode="drop")
        return flat_grid, None

    start_grid = jnp.zeros((grid_cells,), jnp.float32)
    flat_grid, unused = lax.scan(add_batch, start_grid, jnp.arange(slot_count // batch_size, dtype=jnp.int32))
    return flat_grid


def reference(fine_cells, fine_exponent, fine_charge, fine_offset, wide_cells, wide_exponent, wide_charge, wide_offset):
    fine_flat = deposit(fine_cells, fine_exponent, fine_charge, fine_offset, 0, 2)
    level_zero = ROWS * GRID * GRID
    finest_grid = fine_flat[:level_zero].reshape(ROWS, GRID, GRID)
    second_grid = fine_flat[level_zero:].reshape(ROWS // 2, GRID // 2, GRID // 2)
    wide_flat = deposit(wide_cells, wide_exponent, wide_charge, wide_offset, 2, 3)
    outputs = []
    first_cell = 0
    for level_index in range(2, 5):
        rows_here = ROWS >> level_index
        period = GRID >> level_index
        outputs.append(wide_flat[first_cell:first_cell + rows_here * period * period].reshape(rows_here, period * period))
        first_cell += rows_here * period * period
    return (finest_grid, second_grid, outputs[0], outputs[1], outputs[2])
```

```python
import functools

import jax
import jax.numpy as jnp
from jax import lax
from jax.experimental import pallas as pl
from jax.experimental.pallas import tpu as pltpu
from jax.sharding import PartitionSpec as P

GRID = 512
ROWS = 128
HALF = 4
SPILL = 384
WIDE_BLOCK = 2048
DIRECTIONS = [(i, j) for i in (-1, 0, 1) for j in (-1, 0, 1) if (i, j) != (0, 0)]
MESH = pl.DeviceIdType.MESH
F32 = jnp.float32
BF16 = jnp.bfloat16
I32 = jnp.int32


def exchange_kernel(bricks, reps, subs, *refs):
    fine_in, wide_in = refs[0:4], refs[4:8]
    fine_out, wide_out = refs[8:12], refs[12:16]
    fine_send, fine_recv, wide_send, wide_recv, own_sem = refs[16:]
    columns = reps * subs
    devices = bricks * columns
    brick = lax.axis_index("brick")
    column = lax.axis_index("rep") * subs + lax.axis_index("sub")
    me = brick * columns + column
    slots = fine_in[0].shape[1]
    wide_slots = wide_in[0].shape[1]

    def place(brick_at, column_at):
        return {"brick": brick_at, "rep": column_at // subs, "sub": column_at % subs}

    def other(step):
        at = lax.rem(me + step, devices)
        return place(at // columns, lax.rem(at, columns))

    own = []
    for k in range(4):
        spot = wide_out[k].at[:, pl.ds(pl.multiple_of(me * wide_slots, wide_slots), wide_slots)]
        own.append(pltpu.make_async_copy(wide_in[k], spot, own_sem.at[k]))
        own[-1].start()

    barrier = pltpu.get_barrier_semaphore()

    @pl.loop(1, devices)
    def _(step):
        pl.semaphore_signal(barrier, inc=1, device_id=other(step), device_id_type=MESH)

    pl.semaphore_wait(barrier, devices - 1)

    def fine_copy(direction, k):
        up, across = DIRECTIONS[direction]
        target = place(brick + up, lax.rem(column + across + columns, columns))
        slot = 7 - direction
        return pltpu.make_async_remote_copy(
            src_ref=fine_in[k],
            dst_ref=fine_out[k].at[:, pl.ds(slot * slots, slots)],
            send_sem=fine_send.at[direction, k],
            recv_sem=fine_recv.at[slot, k],
            device_id=target,
            device_id_type=MESH,
        )

    def exists(direction):
        up = DIRECTIONS[direction][0]
        return jnp.logical_and(brick + up >= 0, brick + up < bricks)

    for direction in (0, 2, 5, 7, 1, 6, 3, 4):

        @pl.when(exists(direction))
        def _():
            for k in range(4):
                fine_copy(direction, k).start()

    def wide_copy(step, k):
        return pltpu.make_async_remote_copy(
            src_ref=wide_in[k],
            dst_ref=wide_out[k].at[:, pl.ds(pl.multiple_of(me * wide_slots, wide_slots), wide_slots)],
            send_sem=wide_send.at[step, k],
            recv_sem=wide_recv.at[step, k],
            device_id=other(step),
            device_id_type=MESH,
        )

    @pl.loop(1, devices)
    def _(step):
        for k in range(4):
            wide_copy(step, k).start()

    for direction in range(8):

        @pl.when(exists(direction))
        def _():
            for k in range(4):
                fine_copy(direction, k).wait_send()
                pltpu.make_async_copy(
                    fine_in[k],
                    fine_out[k].at[:, pl.ds(direction * slots, slots)],
                    fine_recv.at[direction, k],
                ).wait()

    @pl.loop(1, devices)
    def _(step):
        for k in range(4):
            wide_copy(step, k).wait()

    for k in range(4):
        own[k].wait()


def exchange(mesh_shape, fine, wide):
    bricks, reps, subs = (mesh_shape[name] for name in ("brick", "rep", "sub"))
    devices = bricks * reps * subs
    outs = [jax.ShapeDtypeStruct((a.shape[0], 8 * a.shape[1]), a.dtype) for a in fine]
    outs += [jax.ShapeDtypeStruct((a.shape[0], devices * a.shape[1]), a.dtype) for a in wide]
    vmem = pl.BlockSpec(memory_space=pltpu.VMEM)
    got = pl.pallas_call(
        functools.partial(exchange_kernel, bricks, reps, subs),
        out_shape=outs,
        in_specs=[vmem] * 8,
        out_specs=[vmem] * 8,
        scratch_shapes=[
            pltpu.SemaphoreType.DMA((8, 4)),
            pltpu.SemaphoreType.DMA((8, 4)),
            pltpu.SemaphoreType.DMA((devices, 4)),
            pltpu.SemaphoreType.DMA((devices, 4)),
            pltpu.SemaphoreType.DMA((4,)),
        ],
        compiler_params=pltpu.CompilerParams(collective_id=0, has_side_effects=True),
        name="exchange",
    )(*fine, *wide)
    return got[:4], got[4:]


def factor(cells, centre, radius, exponent, shift, period=None):
    gap = cells - centre
    if period is not None:
        gap = ((gap + period // 2) & (period - 1)) - period // 2
    spread = gap.astype(F32) - shift
    return jnp.where(jnp.abs(gap) <= radius, jnp.exp(-exponent * spread * spread), 0.0)


def stack_rows(cells, offset, exponent, charge):
    pad = jnp.zeros((6, exponent.shape[1]), F32)
    return jnp.concatenate([cells.astype(F32), offset, exponent, charge, pad], 0)


def row_pieces(table, level):
    whole = table[0:5].astype(I32)
    charge = jnp.where(whole[0:1] == level, table[9:10], 0.0)
    return whole[1:2], whole[2:3], whole[3:4], table[5:6], table[6:7], table[8:9], charge


def row_column_factors(table, level, rows, row_start, columns, column_start, period):
    radius, c0, c1, s0, s1, exponent, charge = row_pieces(table, level)
    count = table.shape[1]
    row_cells = row_start + lax.broadcasted_iota(I32, (rows, count), 0)
    col_cells = column_start + lax.broadcasted_iota(I32, (columns, count), 0)
    row_weight = charge * factor(row_cells, c0, radius, exponent, s0)
    col_factor = factor(col_cells, c1, radius, exponent, s1, period)
    return row_weight, col_factor


def depth_factor(turned, period, width):
    whole = turned[:, 0:5].astype(I32)
    cells = lax.broadcasted_iota(I32, (turned.shape[0], width), 1)
    return factor(
        cells, whole[:, 4:5], whole[:, 1:2], turned[:, 8:9], turned[:, 7:8], period
    ).astype(BF16)


def matmul(left, right):
    return jnp.dot(left, right, preferred_element_type=F32)


def collocate_kernel(bricks, columns_n, subs, steps, *refs):
    fine, near, wide = refs[0:4], refs[4:8], refs[8:12]
    out0, out1, out2, out3, out4 = refs[12:17]
    place, depth0, depth1, col0, col1, row0, row1 = refs[17:24]
    spread_at, chunks, wide_depth, wide_depth4 = refs[24:28]
    wide_cols, wide_rows = refs[28:31], refs[31:34]
    brick = lax.axis_index("brick")
    column = lax.axis_index("rep") * subs + lax.axis_index("sub")
    own_slots = fine[0].shape[1]
    outs = (out0, out1)
    row_tiles = [(ROWS >> level) // bricks for level in range(2)]
    col_tiles = [(GRID >> level) // columns_n for level in range(2)]
    periods = [GRID >> level for level in range(2)]
    depths, cols, rows = (depth0, depth1), (col0, col1), (row0, row1)

    def source(refs4, at, count):
        span = pl.ds(at, count)
        return stack_rows(refs4[0][:, span], refs4[3][:, span], refs4[1][:, span], refs4[2][:, span])

    def gather_spill(chunk):
        total = jnp.zeros((48, SPILL), F32)
        slots = lax.broadcasted_iota(I32, (SPILL, own_slots), 0).astype(F32) + (chunk * SPILL).astype(F32)
        for s in range(8):
            where_to = spread_at[s : s + 1, :]
            values = jnp.where(where_to >= 0, source(near, s * own_slots, own_slots), 0.0)
            high = values.astype(BF16)
            rest = values - high.astype(F32)
            middle = rest.astype(BF16)
            low = (rest - middle.astype(F32)).astype(BF16)
            pieces = jnp.concatenate([high, middle, low], 0)
            chosen = jnp.where(where_to == slots, 1.0, 0.0).astype(BF16)
            total += lax.dot_general(
                pieces, chosen, (((1,), (1,)), ((), ())), preferred_element_type=F32
            )
        return total[0:16] + total[16:32] + total[32:48]

    def level_factors(table, level):
        return row_column_factors(
            table,
            level,
            row_tiles[level],
            brick * row_tiles[level],
            col_tiles[level],
            column * col_tiles[level],
            periods[level],
        )

    def spill_places():
        def lined(k):
            return jnp.concatenate(
                [near[0][k : k + 1, s * own_slots : (s + 1) * own_slots] for s in range(8)], 0
            )

        level, radius, c0, c1 = (lined(k) for k in range(4))
        first = level == 0
        row_tile = jnp.where(first, row_tiles[0], row_tiles[1])
        col_tile = jnp.where(first, col_tiles[0], col_tiles[1])
        period = jnp.where(first, periods[0], periods[1])
        across = c0 - brick * row_tile
        along = ((c1 - column * col_tile + period // 2) & (period - 1)) - period // 2
        line = lax.broadcasted_iota(I32, level.shape, 0)
        up = jnp.where(line < 3, -1, jnp.where(line < 5, 0, 1)) + brick
        keep = (up >= 0) & (up < bricks)
        keep &= (across >= -radius) & (across < row_tile + radius)
        wrap = along + period
        keep &= ((along >= -radius) & (along < col_tile + radius)) | (wrap < col_tile + radius)
        keep = jnp.where(keep, 1.0, 0.0)
        count = own_slots // 128
        piled = jnp.concatenate([keep[:, i * 128 : (i + 1) * 128] for i in range(count)], 0)
        height = piled.shape[0]
        upper = lax.broadcasted_iota(I32, (128, 128), 0) <= lax.broadcasted_iota(I32, (128, 128), 1)
        within = matmul(piled.astype(BF16), jnp.where(upper, 1.0, 0.0).astype(BF16))
        sums = jnp.broadcast_to(within[:, 127:128], (height, 128))
        lower = lax.broadcasted_iota(I32, (height, height), 0) > lax.broadcasted_iota(
            I32, (height, height), 1
        )
        before = matmul(jnp.where(lower, 1.0, 0.0).astype(BF16), sums.astype(BF16))
        at = jnp.where(piled > 0.0, before + within - 1.0, -1.0)
        for i in range(count):
            spread_at[:, i * 128 : (i + 1) * 128] = at[i * 8 : (i + 1) * 8]
        chunks[0] = (jnp.max(at).astype(I32) + SPILL) // SPILL

    @pl.when(pl.program_id(0) == 0)
    def _():
        spill_places()
        place[:, 0:own_slots] = source(fine, 0, own_slots)
        place[:, own_slots:] = gather_spill(jnp.int32(0))
        table = place[...]
        turned = table.T
        for level in range(2):
            row_weight, col_factor = level_factors(table, level)
            rows[level][...] = row_weight
            cols[level][...] = col_factor
            depths[level][...] = depth_factor(turned, periods[level], periods[level])
        wide_total = wide[0].shape[1]
        block = wide_cols[0].shape[1]
        for ref in (out2, out3, out4):
            ref[...] = jnp.zeros(ref.shape, F32)

        @pl.loop(0, wide_total // block)
        def _(part):
            wide_table = source(wide, pl.multiple_of(part * block, block), block)
            wide_turned = wide_table.T
            for at, level in enumerate((2, 3, 4)):
                period = GRID >> level
                share = period // bricks
                row_weight, col_factor = row_column_factors(
                    wide_table, level, ROWS >> level, 0, share, brick * share, period
                )
                wide_rows[at][...] = row_weight
                wide_cols[at][...] = col_factor
            wide_depth[:, 0:128] = depth_factor(wide_turned, GRID >> 2, 128)
            wide_depth[:, 128:256] = depth_factor(wide_turned, GRID >> 3, 128)
            wide_depth4[...] = depth_factor(wide_turned, GRID >> 4, 128)
            for at, level, out, depth in (
                (0, 2, out2, wide_depth[:, 0:128]),
                (1, 3, out3, wide_depth[:, 128:256]),
                (2, 4, out4, wide_depth4[...]),
            ):
                period = GRID >> level
                height = ROWS >> level
                share = period // bricks
                group = min(share, 8)

                copies = 128 // period
                for first in range(0, share, group):
                    weights = jnp.concatenate(
                        [
                            (wide_rows[at][...] * wide_cols[at][first + i : first + i + 1, :]).astype(BF16)
                            for i in range(group)
                        ],
                        0,
                    )
                    result = matmul(weights, depth)
                    for i in range(0, group, copies):
                        lane = lax.broadcasted_iota(I32, (height, 128), 1) // period
                        piece = result[i * height : (i + 1) * height]
                        for j in range(1, min(copies, group)):
                            piece = jnp.where(lane == j, result[(i + j) * height : (i + j + 1) * height], piece)
                        width = min(copies, group) * period
                        start = (first + i) * period
                        out[:, start : start + width] += piece[:, 0:width]

    step = pl.program_id(0)

    def slab(level, row_ref, col_value, depth_value, first_row):
        per = row_tiles[level] // steps
        weights = jnp.concatenate(
            [(row_ref(first_row + i) * col_value).astype(BF16) for i in range(per)], 0
        )
        result = matmul(weights, depth_value)
        return result.reshape(per, col_tiles[level], periods[level])

    for level in range(2):
        per = row_tiles[level] // steps
        outs[level][...] = slab(
            level,
            lambda r: rows[level][pl.ds(r, 1), :],
            cols[level][...],
            depths[level][...],
            step * per,
        )

    def extra(chunk, carry):
        table = gather_spill(chunk)
        turned = table.T
        for level in range(2):
            row_weight, col_factor = level_factors(table, level)
            rows[level][:, 0:SPILL] = row_weight
            depth_value = depth_factor(turned, periods[level], periods[level])
            per = row_tiles[level] // steps
            outs[level][...] += slab(
                level, lambda r: rows[level][pl.ds(r, 1), 0:SPILL], col_factor, depth_value, step * per
            )
        return carry

    @pl.when(chunks[0] > 1)
    def _():
        saved = [rows[level][:, 0:SPILL] for level in range(2)]
        lax.fori_loop(1, chunks[0], extra, 0)
        for level in range(2):
            rows[level][:, 0:SPILL] = saved[level]


def collocate(mesh_shape, fine, near, wide):
    bricks, reps, subs = (mesh_shape[name] for name in ("brick", "rep", "sub"))
    columns_n = reps * subs
    row_tiles = [(ROWS >> level) // bricks for level in range(2)]
    col_tiles = [(GRID >> level) // columns_n for level in range(2)]
    periods = [GRID >> level for level in range(2)]
    steps = min(8, row_tiles[1])
    count = fine[0].shape[1] + SPILL
    block = min(WIDE_BLOCK, wide[0].shape[1])

    def whole(shape):
        return pl.BlockSpec(shape, lambda i: (0,) * len(shape))

    shapes = [(row_tiles[level], col_tiles[level], periods[level]) for level in range(2)]
    shapes += [(ROWS >> level, (GRID >> level) ** 2 // bricks) for level in (2, 3, 4)]
    out_specs = [
        pl.BlockSpec((shape[0] // steps,) + shape[1:], lambda i: (i, 0, 0)) for shape in shapes[:2]
    ] + [whole(shape) for shape in shapes[2:]]
    scratch = [
        pltpu.VMEM((16, count), F32),
        pltpu.VMEM((count, periods[0]), BF16),
        pltpu.VMEM((count, periods[1]), BF16),
        pltpu.VMEM((col_tiles[0], count), F32),
        pltpu.VMEM((col_tiles[1], count), F32),
        pltpu.VMEM((row_tiles[0], count), F32),
        pltpu.VMEM((row_tiles[1], count), F32),
        pltpu.VMEM((8, fine[0].shape[1]), F32),
        pltpu.SMEM((1,), I32),
        pltpu.VMEM((block, 256), BF16),
        pltpu.VMEM((block, 128), BF16),
    ]
    scratch += [pltpu.VMEM(((GRID >> level) // bricks, block), F32) for level in (2, 3, 4)]
    scratch += [pltpu.VMEM((ROWS >> level, block), F32) for level in (2, 3, 4)]
    operands = (*fine, *near, *wide)
    return pl.pallas_call(
        functools.partial(collocate_kernel, bricks, columns_n, subs, steps),
        grid=(steps,),
        out_shape=[jax.ShapeDtypeStruct(shape, F32) for shape in shapes],
        in_specs=[whole(a.shape) for a in operands],
        out_specs=out_specs,
        scratch_shapes=scratch,
        compiler_params=pltpu.CompilerParams(
            dimension_semantics=("arbitrary",), vmem_limit_bytes=56 * 1024 * 1024
        ),
        name="collocate",
    )(*operands)


def solution(mesh):
    shape = dict(mesh.shape)

    def per_device(
        fine_cells,
        fine_exponent,
        fine_charge,
        fine_offset,
        wide_cells,
        wide_exponent,
        wide_charge,
        wide_offset,
    ):
        fine = (fine_cells, fine_exponent[None, :], fine_charge[None, :], fine_offset)
        wide = (wide_cells, wide_exponent[None, :], wide_charge[None, :], wide_offset)
        near, wide_all = exchange(shape, fine, wide)
        return tuple(collocate(shape, fine, near, wide_all))

    split = P(("parts", "brick", "rep", "sub"))
    table = P(None, ("parts", "brick", "rep", "sub"))
    return jax.shard_map(
        per_device,
        mesh=mesh,
        in_specs=(table, split, split, table, table, split, split, table),
        out_specs=(
            P(("parts", "brick"), ("rep", "sub"), None),
            P(("parts", "brick"), ("rep", "sub"), None),
            P("parts", "brick"),
            P("parts", "brick"),
            P("parts", "brick"),
        ),
        check_vma=False,
    )
```

```python
import functools

import jax
import jax.numpy as jnp
from jax import lax
from jax.experimental import pallas as pl
from jax.experimental.pallas import tpu as pltpu
from jax.sharding import PartitionSpec as P

GRID = 512
ROWS = 128
HALF = 4
SPILL = 384
WIDE_BLOCK = 256
DIRECTIONS = [(i, j) for i in (-1, 0, 1) for j in (-1, 0, 1) if (i, j) != (0, 0)]
MESH = pl.DeviceIdType.MESH
F32 = jnp.float32
BF16 = jnp.bfloat16
I32 = jnp.int32


def exchange_kernel(bricks, reps, subs, *refs):
    fine_in, wide_in = refs[0:4], refs[4:8]
    fine_out, wide_out = refs[8:12], refs[12:16]
    fine_send, fine_recv, wide_send, wide_recv, own_sem = refs[16:]
    columns = reps * subs
    devices = bricks * columns
    brick = lax.axis_index("brick")
    column = lax.axis_index("rep") * subs + lax.axis_index("sub")
    me = brick * columns + column
    slots = fine_in[0].shape[1]
    wide_slots = wide_in[0].shape[1]

    def place(brick_at, column_at):
        return {"brick": brick_at, "rep": column_at // subs, "sub": column_at % subs}

    def other(step):
        at = lax.rem(me + step, devices)
        return place(at // columns, lax.rem(at, columns))

    own = []
    for k in range(4):
        spot = wide_out[k].at[:, pl.ds(pl.multiple_of(me * wide_slots, wide_slots), wide_slots)]
        own.append(pltpu.make_async_copy(wide_in[k], spot, own_sem.at[k]))
        own[-1].start()

    barrier = pltpu.get_barrier_semaphore()

    @pl.loop(1, devices)
    def _(step):
        pl.semaphore_signal(barrier, inc=1, device_id=other(step), device_id_type=MESH)

    pl.semaphore_wait(barrier, devices - 1)

    def fine_copy(direction, k):
        up, across = DIRECTIONS[direction]
        target = place(brick + up, lax.rem(column + across + columns, columns))
        slot = 7 - direction
        return pltpu.make_async_remote_copy(
            src_ref=fine_in[k],
            dst_ref=fine_out[k].at[:, pl.ds(slot * slots, slots)],
            send_sem=fine_send.at[direction, k],
            recv_sem=fine_recv.at[slot, k],
            device_id=target,
            device_id_type=MESH,
        )

    def exists(direction):
        up = DIRECTIONS[direction][0]
        return jnp.logical_and(brick + up >= 0, brick + up < bricks)

    for direction in (0, 2, 5, 7, 1, 6, 3, 4):

        @pl.when(exists(direction))
        def _():
            for k in range(4):
                fine_copy(direction, k).start()

    def wide_copy(step, k):
        return pltpu.make_async_remote_copy(
            src_ref=wide_in[k],
            dst_ref=wide_out[k].at[:, pl.ds(pl.multiple_of(me * wide_slots, wide_slots), wide_slots)],
            send_sem=wide_send.at[step, k],
            recv_sem=wide_recv.at[step, k],
            device_id=other(step),
            device_id_type=MESH,
        )

    @pl.loop(1, devices)
    def _(step):
        for k in range(4):
            wide_copy(step, k).start()

    for direction in range(8):

        @pl.when(exists(direction))
        def _():
            for k in range(4):
                fine_copy(direction, k).wait_send()
                pltpu.make_async_copy(
                    fine_in[k],
                    fine_out[k].at[:, pl.ds(direction * slots, slots)],
                    fine_recv.at[direction, k],
                ).wait()

    @pl.loop(1, devices)
    def _(step):
        for k in range(4):
            wide_copy(step, k).wait()

    for k in range(4):
        own[k].wait()


def exchange(mesh_shape, fine, wide):
    bricks, reps, subs = (mesh_shape[name] for name in ("brick", "rep", "sub"))
    devices = bricks * reps * subs
    outs = [jax.ShapeDtypeStruct((a.shape[0], 8 * a.shape[1]), a.dtype) for a in fine]
    outs += [jax.ShapeDtypeStruct((a.shape[0], devices * a.shape[1]), a.dtype) for a in wide]
    vmem = pl.BlockSpec(memory_space=pltpu.VMEM)
    got = pl.pallas_call(
        functools.partial(exchange_kernel, bricks, reps, subs),
        out_shape=outs,
        in_specs=[vmem] * 8,
        out_specs=[vmem] * 8,
        scratch_shapes=[
            pltpu.SemaphoreType.DMA((8, 4)),
            pltpu.SemaphoreType.DMA((8, 4)),
            pltpu.SemaphoreType.DMA((devices, 4)),
            pltpu.SemaphoreType.DMA((devices, 4)),
            pltpu.SemaphoreType.DMA((4,)),
        ],
        compiler_params=pltpu.CompilerParams(collective_id=0, has_side_effects=True),
        name="exchange",
    )(*fine, *wide)
    return got[:4], got[4:]


def factor(cells, centre, radius, exponent, shift, period=None):
    gap = cells - centre
    if period is not None:
        half = period // 2
        gap = ((gap + half) & (period - 1)) - half
    spread = gap.astype(F32) - shift
    return jnp.where(jnp.abs(gap) <= radius, jnp.exp(-exponent * spread * spread), 0.0)


def stack_rows(cells, offset, exponent, charge):
    pad = jnp.zeros((6, exponent.shape[1]), F32)
    return jnp.concatenate([cells.astype(F32), offset, exponent, charge, pad], 0)


def halved(size, level):
    return lax.shift_right_logical(jnp.full(level.shape, size, I32), level)


def row_column_factors(table, rows, row_tile, row_block, columns, col_tile, col_block):
    whole = table[0:5].astype(I32)
    level, radius = whole[0:1], whole[1:2]
    exponent, charge = table[8:9], table[9:10]
    count = table.shape[1]
    row_cells = lax.broadcasted_iota(I32, (rows, count), 0)
    col_cells = lax.broadcasted_iota(I32, (columns, count), 0)
    row_centre = whole[2:3] - row_block * halved(row_tile, level)
    col_centre = whole[3:4] - col_block * halved(col_tile, level)
    row_weight = charge * factor(row_cells, row_centre, radius, exponent, table[5:6])
    col_factor = factor(
        col_cells, col_centre, radius, exponent, table[6:7], halved(GRID, level)
    )
    return level, row_weight, col_factor


def depth_factor(turned, width):
    whole = turned[:, 0:5].astype(I32)
    cells = lax.broadcasted_iota(I32, (turned.shape[0], width), 1)
    return factor(
        cells,
        whole[:, 4:5],
        whole[:, 1:2],
        turned[:, 8:9],
        turned[:, 7:8],
        halved(GRID, whole[:, 0:1]),
    ).astype(BF16)


def matmul(left, right):
    return jnp.dot(left, right, preferred_element_type=F32)


def collocate_kernel(bricks, columns_n, subs, steps, wide_block, *refs):
    fine, near, wide = refs[0:4], refs[4:8], refs[8:12]
    out0, out1, out2, out3, out4 = refs[12:17]
    depth, cols, row0, row1, spread_at, chunks = refs[17:]
    brick = lax.axis_index("brick")
    column = lax.axis_index("rep") * subs + lax.axis_index("sub")
    own_slots = fine[0].shape[1]
    outs = (out0, out1)
    row_tiles = [(ROWS >> level) // bricks for level in range(2)]
    col_tiles = [(GRID >> level) // columns_n for level in range(2)]
    periods = [GRID >> level for level in range(2)]
    rows = (row0, row1)

    def source(refs4, at, count):
        span = pl.ds(at, count)
        return stack_rows(refs4[0][:, span], refs4[3][:, span], refs4[1][:, span], refs4[2][:, span])

    def gather_spill(chunk):
        total = jnp.zeros((48, SPILL), F32)
        slots = lax.broadcasted_iota(I32, (SPILL, own_slots), 0).astype(F32) + (chunk * SPILL).astype(F32)
        for s in range(8):
            where_to = spread_at[s : s + 1, :]
            values = jnp.where(where_to >= 0, source(near, s * own_slots, own_slots), 0.0)
            high = values.astype(BF16)
            rest = values - high.astype(F32)
            middle = rest.astype(BF16)
            low = (rest - middle.astype(F32)).astype(BF16)
            pieces = jnp.concatenate([high, middle, low], 0)
            chosen = jnp.where(where_to == slots, 1.0, 0.0).astype(BF16)
            total += lax.dot_general(
                pieces, chosen, (((1,), (1,)), ((), ())), preferred_element_type=F32
            )
        return total[0:16] + total[16:32] + total[32:48]

    def fine_factors(table):
        level, row_weight, col_factor = row_column_factors(
            table, row_tiles[0], row_tiles[0], brick, col_tiles[0], col_tiles[0], column
        )
        first = jnp.where(level == 0, row_weight, 0.0)
        second = jnp.where(level == 1, row_weight[0 : row_tiles[1]], 0.0)
        return (first, second), col_factor, depth_factor(table.T, periods[0])

    def spill_places():
        def lined(k):
            return jnp.concatenate(
                [near[0][k : k + 1, s * own_slots : (s + 1) * own_slots] for s in range(8)], 0
            )

        level, radius, c0, c1 = (lined(k) for k in range(4))
        first = level == 0
        row_tile = jnp.where(first, row_tiles[0], row_tiles[1])
        col_tile = jnp.where(first, col_tiles[0], col_tiles[1])
        period = jnp.where(first, periods[0], periods[1])
        across = c0 - brick * row_tile
        along = ((c1 - column * col_tile + period // 2) & (period - 1)) - period // 2
        line = lax.broadcasted_iota(I32, level.shape, 0)
        up = jnp.where(line < 3, -1, jnp.where(line < 5, 0, 1)) + brick
        keep = (up >= 0) & (up < bricks)
        keep &= (across >= -radius) & (across < row_tile + radius)
        wrap = along + period
        keep &= ((along >= -radius) & (along < col_tile + radius)) | (wrap < col_tile + radius)
        keep = jnp.where(keep, 1.0, 0.0)
        count = own_slots // 128
        piled = jnp.concatenate([keep[:, i * 128 : (i + 1) * 128] for i in range(count)], 0)
        height = piled.shape[0]
        upper = lax.broadcasted_iota(I32, (128, 128), 0) <= lax.broadcasted_iota(I32, (128, 128), 1)
        within = matmul(piled.astype(BF16), jnp.where(upper, 1.0, 0.0).astype(BF16))
        sums = jnp.broadcast_to(within[:, 127:128], (height, 128))
        lower = lax.broadcasted_iota(I32, (height, height), 0) > lax.broadcasted_iota(
            I32, (height, height), 1
        )
        before = matmul(jnp.where(lower, 1.0, 0.0).astype(BF16), sums.astype(BF16))
        at = jnp.where(piled > 0.0, before + within - 1.0, -1.0)
        for i in range(count):
            spread_at[:, i * 128 : (i + 1) * 128] = at[i * 8 : (i + 1) * 8]
        chunks[0] = (jnp.max(at).astype(I32) + SPILL) // SPILL

    @pl.when(pl.program_id(0) == 0)
    def _():
        spill_places()
        table = jnp.concatenate([source(fine, 0, own_slots), gather_spill(jnp.int32(0))], 1)
        weights, cols[...], depth[...] = fine_factors(table)
        for level in range(2):
            rows[level][...] = weights[level]
        for ref in (out2, out3, out4):
            ref[...] = jnp.zeros(ref.shape, F32)

    step = pl.program_id(0)

    def wide_part(part):
        table = source(wide, pl.multiple_of(part * wide_block, wide_block), wide_block)
        share = (GRID >> 2) // bricks
        which, row_weight, col_factor = row_column_factors(
            table, ROWS >> 2, ROWS, 0, share, GRID // bricks, brick
        )
        depth_value = depth_factor(table.T, GRID >> 2)
        lanes = GRID >> 2
        for level, out in ((2, out2), (3, out3), (4, out4)):
            period = GRID >> level
            height = ROWS >> level
            share = period // bricks
            group = min(share, 8)
            copies = lanes // period
            width = min(copies, group)
            own = jnp.where(which == level, row_weight[0:height], 0.0)
            lane = lax.broadcasted_iota(I32, (height, lanes), 1) // period
            for first in range(0, share, group):
                weights = jnp.concatenate(
                    [(own * col_factor[i : i + 1]).astype(BF16) for i in range(first, first + group)], 0
                )
                result = matmul(weights, depth_value)
                for i in range(0, group, width):
                    piece = result[i * height : (i + 1) * height]
                    for j in range(1, width):
                        piece = jnp.where(lane == j, result[(i + j) * height : (i + j + 1) * height], piece)
                    start = (first + i) * period
                    out[:, start : start + width * period] += piece[:, 0 : width * period]

    def slab(level, row_ref, col_value, depth_value):
        per = row_tiles[level] // steps
        weights = jnp.concatenate(
            [(row_ref(step * per + i) * col_value).astype(BF16) for i in range(per)], 0
        )
        result = matmul(weights, depth_value)
        return result.reshape(per, col_tiles[level], periods[level])

    for level in range(2):
        outs[level][...] = slab(
            level,
            lambda r: rows[level][pl.ds(r, 1), :],
            cols[0 : col_tiles[level], :],
            depth[:, 0 : periods[level]],
        )

    parts = wide[0].shape[1] // wide_block // steps
    if parts == 1:
        wide_part(step)
    else:

        @pl.loop(0, parts)
        def _(part):
            wide_part(step * parts + part)

    def extra(chunk, carry):
        weights, col_factor, depth_value = fine_factors(gather_spill(chunk))
        for level in range(2):
            rows[level][:, 0:SPILL] = weights[level]
            outs[level][...] += slab(
                level,
                lambda r: rows[level][pl.ds(r, 1), 0:SPILL],
                col_factor[0 : col_tiles[level]],
                depth_value[:, 0 : periods[level]],
            )
        return carry

    @pl.when(chunks[0] > 1)
    def _():
        saved = [rows[level][:, 0:SPILL] for level in range(2)]
        lax.fori_loop(1, chunks[0], extra, 0)
        for level in range(2):
            rows[level][:, 0:SPILL] = saved[level]


def collocate(mesh_shape, fine, near, wide):
    bricks, reps, subs = (mesh_shape[name] for name in ("brick", "rep", "sub"))
    columns_n = reps * subs
    row_tiles = [(ROWS >> level) // bricks for level in range(2)]
    col_tiles = [(GRID >> level) // columns_n for level in range(2)]
    periods = [GRID >> level for level in range(2)]
    steps = min(8, row_tiles[1])
    count = fine[0].shape[1] + SPILL
    block = min(WIDE_BLOCK, wide[0].shape[1] // steps)

    def whole(shape):
        return pl.BlockSpec(shape, lambda i: (0,) * len(shape))

    shapes = [(row_tiles[level], col_tiles[level], periods[level]) for level in range(2)]
    shapes += [(ROWS >> level, (GRID >> level) ** 2 // bricks) for level in (2, 3, 4)]
    out_specs = [
        pl.BlockSpec((shape[0] // steps,) + shape[1:], lambda i: (i, 0, 0)) for shape in shapes[:2]
    ] + [whole(shape) for shape in shapes[2:]]
    scratch = [
        pltpu.VMEM((count, periods[0]), BF16),
        pltpu.VMEM((col_tiles[0], count), F32),
        pltpu.VMEM((row_tiles[0], count), F32),
        pltpu.VMEM((row_tiles[1], count), F32),
        pltpu.VMEM((8, fine[0].shape[1]), F32),
        pltpu.SMEM((1,), I32),
    ]
    operands = (*fine, *near, *wide)
    return pl.pallas_call(
        functools.partial(collocate_kernel, bricks, columns_n, subs, steps, block),
        grid=(steps,),
        out_shape=[jax.ShapeDtypeStruct(shape, F32) for shape in shapes],
        in_specs=[whole(a.shape) for a in operands],
        out_specs=out_specs,
        scratch_shapes=scratch,
        compiler_params=pltpu.CompilerParams(
            dimension_semantics=("arbitrary",), vmem_limit_bytes=56 * 1024 * 1024
        ),
        name="collocate",
    )(*operands)


def solution(mesh):
    shape = dict(mesh.shape)

    def per_device(
        fine_cells,
        fine_exponent,
        fine_charge,
        fine_offset,
        wide_cells,
        wide_exponent,
        wide_charge,
        wide_offset,
    ):
        fine = (fine_cells, fine_exponent[None, :], fine_charge[None, :], fine_offset)
        wide = (wide_cells, wide_exponent[None, :], wide_charge[None, :], wide_offset)
        near, wide_all = exchange(shape, fine, wide)
        return tuple(collocate(shape, fine, near, wide_all))

    split = P(("parts", "brick", "rep", "sub"))
    table = P(None, ("parts", "brick", "rep", "sub"))
    return jax.shard_map(
        per_device,
        mesh=mesh,
        in_specs=(table, split, split, table, table, split, split, table),
        out_specs=(
            P(("parts", "brick"), ("rep", "sub"), None),
            P(("parts", "brick"), ("rep", "sub"), None),
            P("parts", "brick"),
            P("parts", "brick"),
            P("parts", "brick"),
        ),
        check_vma=False,
    )
```
